32 devices in a mesh: gx: 4 (over x, core), gy: 4 (over z), gz: 2 (over y).
Axes of the slice: x: 2, y: 2, z: 4, core: 2. Of those that a mesh axis runs over, the one named last changes fastest.
Arguments:
- fields: float32 [11, 500, 32, 256], P(None, 'gx', 'gy', 'gz'), may hold values from -6 to 6
- var_scale: float32 [11], replicated, may hold values from 0.3 to 3
- start_basis: float32 [500, 64], replicated, may hold values from -6 to 6
Outputs:
- factor: float32 [500, 64], replicated
- core: float32 [64, 11, 32, 256], P('gx', None, 'gy', 'gz')
The draws below stay inside these ranges and needn't reach their ends.
All inputs are finite; a program needn't handle non-finite values.
Results may differ from the reference program's by a relative error of at most 0.0002.
Values sent between devices are 32-bit elements; how exact they have to be, the bound alone decides.
A program may use at most 128 MiB of HBM per device.

```python
import math
import jax
import jax.numpy as jnp
from jax import lax

V = 11
N1 = 500
RANK = 64
ITERS = 3
N2 = 32
N3 = 256


def steps_of(stream_key, dims, shards, low, largest):
    def one(dim, shards_of):
        heights = jax.random.uniform(jax.random.fold_in(jax.random.fold_in(stream_key, 6), dim), (shards_of,), jnp.float32, low / len(shards), largest / len(shards))
        return jnp.repeat(jnp.exp(heights), dims[dim] // shards_of).reshape((-1,) + (1,) * (len(dims) - dim - 1))

    level = one(*shards[0])
    for cut in shards[1:]:
        level = level * one(*cut)
    return level


def centred(key, shape, width, limit, split=(), dtype=jnp.bfloat16):
    array = jax.random.normal(key, shape, jnp.float32) * width
    if len(split) > 0:
        array = steps_of(key, shape, split, -0.22, 0.18) * array
    return jnp.clip(array, min=-limit, max=limit).astype(dtype)


def setup_inputs(seed: int = 0) -> dict:
    splits = jax.random.split(jax.random.key(seed), 4)
    fields = centred(splits[0], (V, N1, N2, N3), 1.0, 6.0, ((1, 4), (2, 4), (3, 2)), jnp.float32)
    var_scale = jnp.clip(jnp.exp(jax.random.uniform(splits[1], (V,), jnp.float32, math.log(0.3), math.log(3.0))), 0.3, 3.0)
    start_basis = centred(splits[2], (N1, RANK), 1.0, 6.0, (), jnp.float32)
    return dict(fields=fields, var_scale=var_scale, start_basis=start_basis)


def orthonormal(block):
    small = jnp.dot(block.T, block, precision=lax.Precision.HIGHEST)
    lower = jnp.linalg.cholesky(small)
    return jax.scipy.linalg.solve_triangular(lower, block.T, lower=True).T

def reference(fields, var_scale, start_basis):
    scaled = fields * var_scale[:, None, None, None]
    gram = lax.dot_general(scaled, scaled, (((0, 2, 3), (0, 2, 3)), ((), ())), precision=lax.Precision.HIGHEST)
    basis = start_basis
    for step in range(ITERS):
        basis = orthonormal(jnp.dot(gram, basis, precision=lax.Precision.HIGHEST))
    core = lax.dot_general(basis, scaled, (((0,), (1,)), ((), ())), precision=lax.Precision.HIGHEST)
    return (basis, core)
```

```python
import functools

import jax
import jax.numpy as jnp
from jax import lax
from jax.experimental import pallas as pl
from jax.experimental.pallas import tpu as pltpu
from jax.sharding import PartitionSpec as P

ITERS = 3
LANES = 128
SUB = 8
PANEL = 8
HIGHEST = lax.Precision.HIGHEST
MESH = pl.DeviceIdType.MESH


def flat_index(axes, sizes):
    flat = 0
    for name, size in zip(axes, sizes):
        flat = flat * size + lax.axis_index(name)
    return flat


def coords(flat, sizes):
    out = []
    for size in reversed(sizes):
        out.append(lax.rem(flat, size))
        flat = lax.div(flat, size)
    return tuple(reversed(out))


def reduce_kernel(axes, sizes, owners, rows, g_ref, out_ref, recv, own, s1, r1, s2, r2):
    n = 1
    for size in sizes:
        n *= size
    me = flat_index(axes, sizes)
    barrier = pltpu.get_barrier_semaphore()

    def greet(k, c):
        peer = lax.rem(me + k, n)
        pl.semaphore_signal(barrier, inc=1, device_id=coords(peer, sizes), device_id_type=MESH)
        return c

    lax.fori_loop(1, n, greet, 0)
    pl.semaphore_wait(barrier, n - 1)

    def part(peer):
        return pltpu.make_async_remote_copy(
            src_ref=g_ref.at[peer],
            dst_ref=recv.at[me],
            send_sem=s1.at[peer],
            recv_sem=r1.at[me],
            device_id=coords(peer, sizes),
            device_id_type=MESH,
        )

    def part_from(peer):
        return pltpu.make_async_remote_copy(
            src_ref=g_ref.at[0],
            dst_ref=recv.at[peer],
            send_sem=s1.at[peer],
            recv_sem=r1.at[peer],
            device_id=coords(peer, sizes),
            device_id_type=MESH,
        )

    def whole(peer):
        return pltpu.make_async_remote_copy(
            src_ref=own,
            dst_ref=out_ref.at[me],
            send_sem=s2.at[peer],
            recv_sem=r2.at[me],
            device_id=coords(peer, sizes),
            device_id_type=MESH,
        )

    def whole_from(peer):
        return pltpu.make_async_remote_copy(
            src_ref=own,
            dst_ref=out_ref.at[peer],
            send_sem=s2.at[peer],
            recv_sem=r2.at[peer],
            device_id=coords(peer, sizes),
            device_id_type=MESH,
        )

    def each(do, only_owners):
        def step(k, c):
            peer = lax.rem(me + k, n)
            if only_owners and owners < n:
                pl.when(peer < owners)(lambda: do(peer))
            else:
                do(peer)
            return c

        lax.fori_loop(1, n, step, 0)

    def if_owner(do):
        if owners < n:
            pl.when(me < owners)(do)
        else:
            do()

    each(lambda peer: part(peer).start(), True)

    @if_owner
    def _():
        each(lambda peer: part_from(peer).wait_recv(), False)
        recv[pl.ds(me, 1)] = g_ref[pl.ds(me, 1)]
        own[...] = jnp.sum(recv[...], axis=0)
        each(lambda peer: whole(peer).start(), False)
        out_ref[pl.ds(me, 1)] = own[...][None]

    each(lambda peer: part(peer).wait_send(), True)
    each(lambda peer: whole_from(peer).wait_recv(), True)

    @if_owner
    def _():
        each(lambda peer: whole(peer).wait_send(), False)


def all_reduce_rows(packed, axes, sizes):
    n = 1
    for size in sizes:
        n *= size
    total = packed.shape[0]
    rows = -(-total // (n * SUB)) * SUB
    owners = -(-total // rows)
    packed = jnp.pad(packed, ((0, owners * rows - total), (0, 0))).reshape(owners, rows, LANES)
    out = pl.pallas_call(
        functools.partial(reduce_kernel, axes, sizes, owners, rows),
        out_shape=jax.ShapeDtypeStruct((owners, rows, LANES), jnp.float32),
        in_specs=[pl.BlockSpec(memory_space=pltpu.VMEM)],
        out_specs=pl.BlockSpec(memory_space=pltpu.VMEM),
        scratch_shapes=[
            pltpu.VMEM((n, rows, LANES), jnp.float32),
            pltpu.VMEM((rows, LANES), jnp.float32),
            pltpu.SemaphoreType.DMA((n,)),
            pltpu.SemaphoreType.DMA((n,)),
            pltpu.SemaphoreType.DMA((n,)),
            pltpu.SemaphoreType.DMA((n,)),
        ],
        compiler_params=pltpu.CompilerParams(collective_id=0, has_side_effects=True),
    )(packed)
    return out.reshape(owners * rows, LANES)[:total]


def full(x):
    return jnp.broadcast_to(x, (SUB, LANES))


def inverse_lower(m, rank):
    groups = rank // SUB
    left = LANES - rank
    tiles = [m[g * SUB:(g + 1) * SUB, :] for g in range(groups)]
    sub = lax.broadcasted_iota(jnp.int32, (SUB, LANES), 0)
    done = []
    for g0 in range(groups):
        base = g0 * SUB
        cols = [
            [full(tiles[g][:, left + base + k:left + base + k + 1]) for g in range(g0, groups)]
            for k in range(SUB)
        ]
        rows = [full(tiles[g0][k:k + 1, :]) for k in range(SUB)]
        out = jnp.zeros((SUB, LANES), jnp.float32)
        for a in range(SUB):
            pivot = full(cols[a][0][a:a + 1, :])
            inv = 1.0 / pivot
            row = rows[a] * inv
            out = jnp.where(sub == a, rows[a] * lax.rsqrt(pivot), out)
            for b in range(a + 1, SUB):
                f = full(cols[a][0][b:b + 1, :])
                rows[b] = rows[b] - f * row
                fi = f * inv
                cols[b] = [cb - ca * fi for cb, ca in zip(cols[b], cols[a])]
            for i, g in enumerate(range(g0 + 1, groups)):
                tiles[g] = tiles[g] - cols[a][i + 1] * row
        done.append(out)
    return jnp.concatenate(done, axis=0)[:, :rank]


def iterate_kernel(m, rank, cells, p_ref, start_ref, bt_ref, f_ref, gram, wide):
    t = 0
    for i in range(m):
        for j in range(i, m):
            block = p_ref[t * LANES:(t + 1) * LANES, :]
            gram[i * LANES:(i + 1) * LANES, j * LANES:(j + 1) * LANES] = block
            if i != j:
                gram[j * LANES:(j + 1) * LANES, i * LANES:(i + 1) * LANES] = block.T
            t += 1
    wide[...] = jnp.zeros_like(wide)
    bt_ref[...] = start_ref[...]
    eye = (
        lax.broadcasted_iota(jnp.int32, (rank, LANES), 0)
        == lax.broadcasted_iota(jnp.int32, (rank, LANES), 1)
    ).astype(jnp.float32)

    def step(_, c):
        block = jnp.dot(bt_ref[...], gram[...], precision=HIGHEST, preferred_element_type=jnp.float32)
        wide[LANES - rank:, :] = block
        small = lax.dot_general(
            block, wide[...], (((1,), (1,)), ((), ())), precision=HIGHEST, preferred_element_type=jnp.float32
        )
        lower_inv = inverse_lower(small + eye, rank)
        bt_ref[...] = jnp.dot(lower_inv, block, precision=HIGHEST, preferred_element_type=jnp.float32)
        return c

    lax.fori_loop(0, ITERS, step, 0)
    f_ref[...] = bt_ref[...].T[:cells, :]


def iterate(packed, start_basis, m):
    cells, rank = start_basis.shape
    size = m * LANES
    start = jnp.pad(start_basis.T, ((0, 0), (0, size - cells)))
    vmem = pl.BlockSpec(memory_space=pltpu.VMEM)
    return pl.pallas_call(
        functools.partial(iterate_kernel, m, rank, cells),
        out_shape=(
            jax.ShapeDtypeStruct((rank, size), jnp.float32),
            jax.ShapeDtypeStruct((cells, rank), jnp.float32),
        ),
        in_specs=[vmem, vmem],
        out_specs=(vmem, vmem),
        scratch_shapes=[
            pltpu.VMEM((size, size), jnp.float32),
            pltpu.VMEM((LANES, size), jnp.float32),
        ],
    )(packed, start)


def solution(mesh):
    axes = tuple(mesh.axis_names)
    sizes = tuple(mesh.shape[a] for a in axes)

    def per_device(fields, var_scale, start_basis):
        scaled = fields * var_scale[:, None, None, None]
        contract = (((0, 2, 3), (0, 2, 3)), ((), ()))
        swapped = lax.all_to_all(scaled, "gx", split_axis=2, concat_axis=1, tiled=True)
        partial_gram = lax.dot_general(swapped, swapped, contract, precision=HIGHEST)
        cells = partial_gram.shape[0]
        m = -(-cells // LANES)
        pad = m * LANES - cells
        padded = jnp.pad(partial_gram, ((0, pad), (0, pad)))
        packed = jnp.concatenate(
            [
                padded[i * LANES:(i + 1) * LANES, j * LANES:(j + 1) * LANES]
                for i in range(m)
                for j in range(i, m)
            ],
            axis=0,
        )
        packed = all_reduce_rows(packed, axes, sizes)
        basis_t, factor = iterate(packed, start_basis, m)
        share = lax.dot_general(
            basis_t[:, :cells], swapped, (((1,), (1,)), ((), ())), precision=lax.Precision.HIGH
        )
        core = lax.all_to_all(share, "gx", split_axis=0, concat_axis=2, tiled=True)
        return factor, core

    in_specs = (P(None, "gx", "gy", "gz"), P(), P())
    out_specs = (P(), P("gx", None, "gy", "gz"))
    return jax.shard_map(
        per_device, mesh=mesh, in_specs=in_specs, out_specs=out_specs, check_vma=False
    )
```

```python
import functools

import jax
import jax.numpy as jnp
from jax import lax
from jax.experimental import pallas as pl
from jax.experimental.pallas import tpu as pltpu
from jax.sharding import PartitionSpec as P

ITERS = 3
LANES = 128
SUB = 8
PANEL = 8
HIGHEST = lax.Precision.HIGHEST
MESH = pl.DeviceIdType.MESH


def flat_index(axes, sizes):
    flat = 0
    for name, size in zip(axes, sizes):
        flat = flat * size + lax.axis_index(name)
    return flat


def coords(flat, sizes):
    out = []
    for size in reversed(sizes):
        out.append(lax.rem(flat, size))
        flat = lax.div(flat, size)
    return tuple(reversed(out))


def greet(peers):
    barrier = pltpu.get_barrier_semaphore()
    for count, place in peers:
        for k in range(1, count):
            pl.semaphore_signal(barrier, inc=1, device_id=place(k), device_id_type=MESH)
    pl.semaphore_wait(barrier, sum(count - 1 for count, _ in peers))


def send(src, dst, sems, device):
    return pltpu.make_async_remote_copy(
        src_ref=src,
        dst_ref=dst,
        send_sem=sems[0],
        recv_sem=sems[1],
        device_id=device,
        device_id_type=MESH,
    )


def reduce_kernel(axes, sizes, g_ref, out_ref, recv_a, mine, recv_b, own, *sems):
    na, nb = g_ref.shape[0], g_ref.shape[1]
    rest = sizes[1:]
    a = lax.axis_index(axes[0])
    b = flat_index(axes[1:], rest)
    b_at = tuple(lax.axis_index(name) for name in axes[1:])

    def peer_a(k):
        return lax.rem(a + k, na)

    def peer_b(k):
        return lax.rem(b + k, nb)

    def dev_a(k):
        return (peer_a(k),) + b_at

    def dev_b(k):
        return (a,) + coords(peer_b(k), rest)

    greet([(na, dev_a), (nb, dev_b)])
    (s1, r1), (s2, r2), (s3, r3), (s4, r4) = [(sems[2 * i], sems[2 * i + 1]) for i in range(4)]

    first = [send(g_ref.at[peer_a(k)], recv_a.at[k], (s1.at[k], r1.at[k]), dev_a(k)) for k in range(1, na)]
    for copy in first:
        copy.start()
    for copy in first:
        copy.wait_recv()
    total = g_ref[pl.ds(a, 1)][0]
    for k in range(1, na):
        total = total + recv_a[k]
    mine[...] = total

    second = [send(mine.at[peer_b(k)], recv_b.at[k], (s2.at[k], r2.at[k]), dev_b(k)) for k in range(1, nb)]
    for copy in second:
        copy.start()
    for copy in second:
        copy.wait_recv()
    total = mine[pl.ds(b, 1)][0]
    for k in range(1, nb):
        total = total + recv_b[k]
    own[...] = total
    out_ref[pl.ds(a, 1), pl.ds(b, 1)] = total[None, None]

    third = [send(own, out_ref.at[a, b], (s3.at[k], r3.at[k]), dev_b(k)) for k in range(1, nb)]
    for copy in third:
        copy.start()
    for k in range(1, nb):
        came = lax.rem(b + nb - k, nb)
        send(own, out_ref.at[a, came], (s3.at[k], r3.at[k]), dev_b(k)).wait_recv()

    fourth = [send(out_ref.at[a], out_ref.at[a], (s4.at[k], r4.at[k]), dev_a(k)) for k in range(1, na)]
    for copy in fourth:
        copy.start()
    for k in range(1, na):
        came = lax.rem(a + na - k, na)
        send(out_ref.at[a], out_ref.at[came], (s4.at[k], r4.at[k]), dev_a(k)).wait_recv()
    for copy in first + second + third + fourth:
        copy.wait_send()


def all_reduce_rows(packed, axes, sizes):
    na = sizes[0]
    nb = 1
    for size in sizes[1:]:
        nb *= size
    rows = packed.shape[0] // (na * nb)
    block = (rows, LANES)
    dma = pltpu.SemaphoreType.DMA
    out = pl.pallas_call(
        functools.partial(reduce_kernel, axes, sizes),
        out_shape=jax.ShapeDtypeStruct((na, nb) + block, jnp.float32),
        in_specs=[pl.BlockSpec(memory_space=pltpu.VMEM)],
        out_specs=pl.BlockSpec(memory_space=pltpu.VMEM),
        scratch_shapes=[
            pltpu.VMEM((na, nb) + block, jnp.float32),
            pltpu.VMEM((nb,) + block, jnp.float32),
            pltpu.VMEM((nb,) + block, jnp.float32),
            pltpu.VMEM(block, jnp.float32),
            dma((na,)), dma((na,)), dma((nb,)), dma((nb,)),
            dma((nb,)), dma((nb,)), dma((na,)), dma((na,)),
        ],
        compiler_params=pltpu.CompilerParams(collective_id=0, has_side_effects=True),
    )(packed.reshape((na, nb) + block))
    return out.reshape(na * nb * rows, LANES)


def swap_kernel(axes, chunk, t_ref, buf, g_ref, acc, local_sem, send_sem, recv_sem):
    units, na, height = buf.shape[0], buf.shape[1], buf.shape[2]
    size = na * height
    m = size // LANES
    chunks = units // chunk
    a = lax.axis_index(axes[0])
    rest = tuple(lax.axis_index(name) for name in axes[1:])

    def peer(k):
        return lax.rem(a + k, na)

    def dev(k):
        return (peer(k),) + rest

    def go(c, k):
        return send(
            t_ref.at[pl.ds(peer(k) * units + c * chunk, chunk)],
            buf.at[pl.ds(c * chunk, chunk), a],
            (send_sem.at[c, k], recv_sem.at[c, k]),
            dev(k),
        )

    def come(c, k):
        return send(
            t_ref.at[pl.ds(c * chunk, chunk)],
            buf.at[pl.ds(c * chunk, chunk), lax.rem(a + na - k, na)],
            (send_sem.at[c, k], recv_sem.at[c, k]),
            dev(k),
        )

    def stay(c):
        return pltpu.make_async_copy(
            t_ref.at[pl.ds(a * units + c * chunk, chunk)],
            buf.at[pl.ds(c * chunk, chunk), a],
            local_sem.at[c],
        )

    greet([(na, dev)])

    def start(c, x):
        for k in range(1, na):
            go(c, k).start()
        stay(c).start()
        return x

    lax.fori_loop(0, chunks, start, 0)
    acc[...] = jnp.zeros_like(acc)

    def use(c, x):
        for k in range(1, na):
            come(c, k).wait_recv()
        stay(c).wait()
        x = jnp.concatenate(
            [buf[c * chunk + u].reshape(size, LANES) for u in range(chunk)], axis=1
        )
        for i in range(0, m, 2):
            top, low = i * LANES, min(i + 2, m) * LANES
            acc[top:low, top:] += lax.dot_general(
                x[top:low], x[top:], (((1,), (1,)), ((), ())),
                precision=HIGHEST, preferred_element_type=jnp.float32,
            )
        return 0

    lax.fori_loop(0, chunks, use, 0)
    t = 0
    for i in range(m):
        for j in range(i, m):
            g_ref[t * LANES:(t + 1) * LANES, :] = acc[
                i * LANES:(i + 1) * LANES, j * LANES:(j + 1) * LANES
            ]
            t += 1
    if t * LANES < g_ref.shape[0]:
        g_ref[t * LANES:, :] = jnp.zeros((g_ref.shape[0] - t * LANES, LANES), jnp.float32)

    def finish(c, x):
        for k in range(1, na):
            go(c, k).wait_send()
        return x

    lax.fori_loop(0, chunks, finish, 0)


def swap_and_gram(t, axes, sizes):
    na = sizes[0]
    n = 1
    for size in sizes:
        n *= size
    units, height = t.shape[0] // na, t.shape[1]
    m = na * height // LANES
    rows = -(-(m * (m + 1) // 2 * LANES) // (n * SUB)) * SUB
    chunk = 2 if units % 2 == 0 else 1
    vmem = pl.BlockSpec(memory_space=pltpu.VMEM)
    dma = pltpu.SemaphoreType.DMA
    return pl.pallas_call(
        functools.partial(swap_kernel, axes, chunk),
        out_shape=(
            jax.ShapeDtypeStruct((units, na, height, LANES), jnp.float32),
            jax.ShapeDtypeStruct((n * rows, LANES), jnp.float32),
        ),
        in_specs=[pl.BlockSpec(memory_space=pl.ANY)],
        out_specs=(vmem, vmem),
        scratch_shapes=[
            pltpu.VMEM((na * height, na * height), jnp.float32),
            dma((units // chunk,)),
            dma((units // chunk, na)),
            dma((units // chunk, na)),
        ],
        compiler_params=pltpu.CompilerParams(collective_id=1, has_side_effects=True),
    )(t)


def full(x):
    return jnp.broadcast_to(x, (SUB, LANES))


def inverse_lower(m, rank):
    groups = rank // SUB
    left = LANES - rank
    tiles = [m[g * SUB:(g + 1) * SUB, :] for g in range(groups)]
    sub = lax.broadcasted_iota(jnp.int32, (SUB, LANES), 0)
    done = []
    for g0 in range(groups):
        base = g0 * SUB
        cols = [
            [full(tiles[g][:, left + base + k:left + base + k + 1]) for g in range(g0, groups)]
            for k in range(SUB)
        ]
        rows = [full(tiles[g0][k:k + 1, :]) for k in range(SUB)]
        out = jnp.zeros((SUB, LANES), jnp.float32)
        for a in range(SUB):
            pivot = full(cols[a][0][a:a + 1, :])
            inv = 1.0 / pivot
            row = rows[a] * inv
            out = jnp.where(sub == a, rows[a] * lax.rsqrt(pivot), out)
            for b in range(a + 1, SUB):
                f = full(cols[a][0][b:b + 1, :])
                rows[b] = rows[b] - f * row
                fi = f * inv
                cols[b] = [cb - ca * fi for cb, ca in zip(cols[b], cols[a])]
            for i, g in enumerate(range(g0 + 1, groups)):
                tiles[g] = tiles[g] - cols[a][i + 1] * row
        done.append(out)
    return jnp.concatenate(done, axis=0)[:, :rank]


def iterate_kernel(m, rank, parts, p_ref, start_ref, bt_ref, f_ref, gram, wide):
    t = 0
    for i in range(m):
        for j in range(i, m):
            block = p_ref[t * LANES:(t + 1) * LANES, :]
            gram[i * LANES:(i + 1) * LANES, j * LANES:(j + 1) * LANES] = block
            if i != j:
                gram[j * LANES:(j + 1) * LANES, i * LANES:(i + 1) * LANES] = block.T
            t += 1
    wide[...] = jnp.zeros_like(wide)
    bt_ref[...] = start_ref[...]
    eye = (
        lax.broadcasted_iota(jnp.int32, (rank, LANES), 0)
        == lax.broadcasted_iota(jnp.int32, (rank, LANES), 1)
    ).astype(jnp.float32)

    def step(_, c):
        block = jnp.dot(bt_ref[...], gram[...], precision=HIGHEST, preferred_element_type=jnp.float32)
        wide[LANES - rank:, :] = block
        small = lax.dot_general(
            block, wide[...], (((1,), (1,)), ((), ())), precision=HIGHEST, preferred_element_type=jnp.float32
        )
        lower_inv = inverse_lower(small + eye, rank)
        bt_ref[...] = jnp.dot(lower_inv, block, precision=HIGHEST, preferred_element_type=jnp.float32)
        return c

    lax.fori_loop(0, ITERS, step, 0)
    basis = bt_ref[...].T
    height, cells = basis.shape[0] // parts, f_ref.shape[0] // parts
    for p in range(parts):
        f_ref[p * cells:(p + 1) * cells, :] = basis[p * height:p * height + cells, :]


def iterate(packed, start_basis, m, parts):
    cells, rank = start_basis.shape
    size = m * LANES
    start = start_basis.T.reshape(rank, parts, cells // parts)
    start = jnp.pad(start, ((0, 0), (0, 0), (0, (size - cells) // parts))).reshape(rank, size)
    vmem = pl.BlockSpec(memory_space=pltpu.VMEM)
    return pl.pallas_call(
        functools.partial(iterate_kernel, m, rank, parts),
        out_shape=(
            jax.ShapeDtypeStruct((rank, size), jnp.float32),
            jax.ShapeDtypeStruct((cells, rank), jnp.float32),
        ),
        in_specs=[vmem, vmem],
        out_specs=(vmem, vmem),
        scratch_shapes=[
            pltpu.VMEM((size, size), jnp.float32),
            pltpu.VMEM((LANES, size), jnp.float32),
        ],
    )(packed, start)


def solution(mesh):
    axes = tuple(mesh.axis_names)
    sizes = tuple(mesh.shape[a] for a in axes)

    def per_device(fields, var_scale, start_basis):
        na = sizes[0]
        nv, cells, nj, nk = fields.shape
        height = -(-cells // LANES) * LANES
        scaled = fields * var_scale[:, None, None, None]
        t = scaled.reshape(nv, cells, na, nj // na, nk).transpose(2, 0, 3, 1, 4)
        t = jnp.pad(t, ((0, 0), (0, 0), (0, 0), (0, height - cells), (0, 0)))
        swapped, packed = swap_and_gram(t.reshape(nv * nj, height, nk), axes, sizes)
        packed = all_reduce_rows(packed, axes, sizes)
        basis_t, factor = iterate(packed, start_basis, na * height // LANES, na)
        share = lax.dot_general(
            basis_t,
            swapped.reshape(-1, na * height, nk),
            (((1,), (1,)), ((), ())),
            precision=lax.Precision.HIGH,
        ).reshape(-1, nv, nj // na, nk)
        core = lax.all_to_all(share, "gx", split_axis=0, concat_axis=2, tiled=True)
        return factor, core

    in_specs = (P(None, "gx", "gy", "gz"), P(), P())
    out_specs = (P(), P("gx", None, "gy", "gz"))
    return jax.shard_map(
        per_device, mesh=mesh, in_specs=in_specs, out_specs=out_specs, check_vma=False
    )
```

```python
import functools

import jax
import jax.numpy as jnp
from jax import lax
from jax.experimental import pallas as pl
from jax.experimental.pallas import tpu as pltpu
from jax.sharding import PartitionSpec as P

ITERS = 3
LANES = 128
SUB = 8
PANEL = 8
HIGHEST = lax.Precision.HIGHEST
MESH = pl.DeviceIdType.MESH


def flat_index(axes, sizes):
    flat = 0
    for name, size in zip(axes, sizes):
        flat = flat * size + lax.axis_index(name)
    return flat


def coords(flat, sizes):
    out = []
    for size in reversed(sizes):
        out.append(lax.rem(flat, size))
        flat = lax.div(flat, size)
    return tuple(reversed(out))


def greet(peers):
    barrier = pltpu.get_barrier_semaphore()
    for count, place in peers:
        for k in range(1, count):
            pl.semaphore_signal(barrier, inc=1, device_id=place(k), device_id_type=MESH)
    pl.semaphore_wait(barrier, sum(count - 1 for count, _ in peers))


def send(src, dst, sems, device):
    return pltpu.make_async_remote_copy(
        src_ref=src,
        dst_ref=dst,
        send_sem=sems[0],
        recv_sem=sems[1],
        device_id=device,
        device_id_type=MESH,
    )


def reduce_kernel(axes, sizes, g_ref, out_ref, recv_a, mine, recv_b, own, *sems):
    na, nb = g_ref.shape[0], g_ref.shape[1]
    rest = sizes[1:]
    a = lax.axis_index(axes[0])
    b = flat_index(axes[1:], rest)
    b_at = tuple(lax.axis_index(name) for name in axes[1:])

    def peer_a(k):
        return lax.rem(a + k, na)

    def peer_b(k):
        return lax.rem(b + k, nb)

    def dev_a(k):
        return (peer_a(k),) + b_at

    def dev_b(k):
        return (a,) + coords(peer_b(k), rest)

    greet([(na, dev_a), (nb, dev_b)])
    (s1, r1), (s2, r2), (s3, r3), (s4, r4) = [(sems[2 * i], sems[2 * i + 1]) for i in range(4)]

    first = [send(g_ref.at[peer_a(k)], recv_a.at[k], (s1.at[k], r1.at[k]), dev_a(k)) for k in range(1, na)]
    for copy in first:
        copy.start()
    for copy in first:
        copy.wait_recv()
    total = g_ref[pl.ds(a, 1)][0]
    for k in range(1, na):
        total = total + recv_a[k]
    mine[...] = total

    second = [send(mine.at[peer_b(k)], recv_b.at[k], (s2.at[k], r2.at[k]), dev_b(k)) for k in range(1, nb)]
    for copy in second:
        copy.start()
    for copy in second:
        copy.wait_recv()
    total = mine[pl.ds(b, 1)][0]
    for k in range(1, nb):
        total = total + recv_b[k]
    own[...] = total
    out_ref[pl.ds(a, 1), pl.ds(b, 1)] = total[None, None]

    third = [send(own, out_ref.at[a, b], (s3.at[k], r3.at[k]), dev_b(k)) for k in range(1, nb)]
    for copy in third:
        copy.start()
    for k in range(1, nb):
        came = lax.rem(b + nb - k, nb)
        send(own, out_ref.at[a, came], (s3.at[k], r3.at[k]), dev_b(k)).wait_recv()

    fourth = [send(out_ref.at[a], out_ref.at[a], (s4.at[k], r4.at[k]), dev_a(k)) for k in range(1, na)]
    for copy in fourth:
        copy.start()
    for k in range(1, na):
        came = lax.rem(a + na - k, na)
        send(out_ref.at[a], out_ref.at[came], (s4.at[k], r4.at[k]), dev_a(k)).wait_recv()
    for copy in first + second + third + fourth:
        copy.wait_send()


def all_reduce_rows(packed, axes, sizes):
    na = sizes[0]
    nb = 1
    for size in sizes[1:]:
        nb *= size
    rows = packed.shape[0] // (na * nb)
    block = (rows, LANES)
    dma = pltpu.SemaphoreType.DMA
    out = pl.pallas_call(
        functools.partial(reduce_kernel, axes, sizes),
        out_shape=jax.ShapeDtypeStruct((na, nb) + block, jnp.float32),
        in_specs=[pl.BlockSpec(memory_space=pltpu.VMEM)],
        out_specs=pl.BlockSpec(memory_space=pltpu.VMEM),
        scratch_shapes=[
            pltpu.VMEM((na, nb) + block, jnp.float32),
            pltpu.VMEM((nb,) + block, jnp.float32),
            pltpu.VMEM((nb,) + block, jnp.float32),
            pltpu.VMEM(block, jnp.float32),
            dma((na,)), dma((na,)), dma((nb,)), dma((nb,)),
            dma((nb,)), dma((nb,)), dma((na,)), dma((na,)),
        ],
        compiler_params=pltpu.CompilerParams(collective_id=0, has_side_effects=True),
    )(packed.reshape((na, nb) + block))
    return out.reshape(na * nb * rows, LANES)


def swap_kernel(axes, chunk, cells, f_ref, scale_ref, buf, g_ref, acc, fbuf, t_ref, load_sem, local_sem, send_sem, recv_sem):
    units, na, height = buf.shape[0], buf.shape[1], buf.shape[2]
    size = na * height
    m = size // LANES
    chunks = units // chunk
    a = lax.axis_index(axes[0])
    rest = tuple(lax.axis_index(name) for name in axes[1:])

    def peer(k):
        return lax.rem(a + k, na)

    def dev(k):
        return (peer(k),) + rest

    def go(c, k):
        return send(
            t_ref.at[c, pl.ds(peer(k) * chunk, chunk)],
            buf.at[pl.ds(c * chunk, chunk), a],
            (send_sem.at[c, k], recv_sem.at[c, k]),
            dev(k),
        )

    def come(c, k):
        return send(
            t_ref.at[c, pl.ds(a * chunk, chunk)],
            buf.at[pl.ds(c * chunk, chunk), lax.rem(a + na - k, na)],
            (send_sem.at[c, k], recv_sem.at[c, k]),
            dev(k),
        )

    def stay(c):
        return pltpu.make_async_copy(
            t_ref.at[c, pl.ds(a * chunk, chunk)],
            buf.at[pl.ds(c * chunk, chunk), a],
            local_sem.at[c],
        )

    nj = na * chunk

    def load(c):
        return pltpu.make_async_copy(f_ref.at[c], fbuf.at[c], load_sem.at[c])

    def fetch(c, x):
        load(c).start()
        return x

    lax.fori_loop(0, chunks, fetch, 0)
    greet([(na, dev)])

    def start(c):
        for k in range(1, na):
            go(c, k).start()
        stay(c).start()

    def turn(c, x):
        load(c).wait()
        scale = scale_ref[c]
        for j in range(nj):
            t_ref[c, j, :cells, :] = fbuf[c, pl.ds(j, cells, stride=nj), :] * scale
            if cells < height:
                t_ref[c, j, cells:, :] = jnp.zeros((height - cells, LANES), jnp.float32)
        pl.when(c > 0)(lambda: start(c - 1))
        return x

    lax.fori_loop(0, chunks, turn, 0)
    start(chunks - 1)
    acc[...] = jnp.zeros_like(acc)

    def use(c, x):
        for k in range(1, na):
            come(c, k).wait_recv()
        stay(c).wait()
        x = jnp.concatenate(
            [buf[c * chunk + u].reshape(size, LANES) for u in range(chunk)], axis=1
        )
        for i in range(0, m, 2):
            top, low = i * LANES, min(i + 2, m) * LANES
            acc[top:low, top:] += lax.dot_general(
                x[top:low], x[top:], (((1,), (1,)), ((), ())),
                precision=HIGHEST, preferred_element_type=jnp.float32,
            )
        return 0

    lax.fori_loop(0, chunks, use, 0)
    t = 0
    for i in range(m):
        for j in range(i, m):
            g_ref[t * LANES:(t + 1) * LANES, :] = acc[
                i * LANES:(i + 1) * LANES, j * LANES:(j + 1) * LANES
            ]
            t += 1
    if t * LANES < g_ref.shape[0]:
        g_ref[t * LANES:, :] = jnp.zeros((g_ref.shape[0] - t * LANES, LANES), jnp.float32)

    def finish(c, x):
        for k in range(1, na):
            go(c, k).wait_send()
        return x

    lax.fori_loop(0, chunks, finish, 0)


def swap_and_gram(fields, var_scale, height, axes, sizes):
    na = sizes[0]
    n = 1
    for size in sizes:
        n *= size
    nv, cells, nj, nk = fields.shape
    chunk = nj // na
    units = nv * chunk
    m = na * height // LANES
    rows = -(-(m * (m + 1) // 2 * LANES) // (n * SUB)) * SUB
    vmem = pl.BlockSpec(memory_space=pltpu.VMEM)
    dma = pltpu.SemaphoreType.DMA
    return pl.pallas_call(
        functools.partial(swap_kernel, axes, chunk, cells),
        out_shape=(
            jax.ShapeDtypeStruct((units, na, height, LANES), jnp.float32),
            jax.ShapeDtypeStruct((n * rows, LANES), jnp.float32),
        ),
        in_specs=[pl.BlockSpec(memory_space=pl.ANY), pl.BlockSpec(memory_space=pltpu.SMEM)],
        out_specs=(vmem, vmem),
        scratch_shapes=[
            pltpu.VMEM((na * height, na * height), jnp.float32),
            pltpu.VMEM((nv, cells * nj, LANES), jnp.float32),
            pltpu.VMEM((nv, nj, height, LANES), jnp.float32),
            dma((nv,)),
            dma((nv,)),
            dma((nv, na)),
            dma((nv, na)),
        ],
        compiler_params=pltpu.CompilerParams(collective_id=1, has_side_effects=True),
    )(fields.reshape(nv, cells * nj, nk), var_scale)


def full(x):
    return jnp.broadcast_to(x, (SUB, LANES))


def inverse_lower(m, rank):
    groups = rank // SUB
    left = LANES - rank
    tiles = [m[g * SUB:(g + 1) * SUB, :] for g in range(groups)]
    sub = lax.broadcasted_iota(jnp.int32, (SUB, LANES), 0)
    done = []
    for g0 in range(groups):
        base = g0 * SUB
        cols = [
            [full(tiles[g][:, left + base + k:left + base + k + 1]) for g in range(g0, groups)]
            for k in range(SUB)
        ]
        rows = [full(tiles[g0][k:k + 1, :]) for k in range(SUB)]
        out = jnp.zeros((SUB, LANES), jnp.float32)
        for a in range(SUB):
            pivot = full(cols[a][0][a:a + 1, :])
            inv = 1.0 / pivot
            row = rows[a] * inv
            out = jnp.where(sub == a, rows[a] * lax.rsqrt(pivot), out)
            for b in range(a + 1, SUB):
                f = full(cols[a][0][b:b + 1, :])
                rows[b] = rows[b] - f * row
                fi = f * inv
                cols[b] = [cb - ca * fi for cb, ca in zip(cols[b], cols[a])]
            for i, g in enumerate(range(g0 + 1, groups)):
                tiles[g] = tiles[g] - cols[a][i + 1] * row
        done.append(out)
    return jnp.concatenate(done, axis=0)[:, :rank]


def iterate_kernel(m, rank, parts, p_ref, start_ref, bt_ref, f_ref, gram, wide):
    t = 0
    for i in range(m):
        for j in range(i, m):
            block = p_ref[t * LANES:(t + 1) * LANES, :]
            gram[i * LANES:(i + 1) * LANES, j * LANES:(j + 1) * LANES] = block
            if i != j:
                gram[j * LANES:(j + 1) * LANES, i * LANES:(i + 1) * LANES] = block.T
            t += 1
    wide[...] = jnp.zeros_like(wide)
    bt_ref[...] = start_ref[...]
    eye = (
        lax.broadcasted_iota(jnp.int32, (rank, LANES), 0)
        == lax.broadcasted_iota(jnp.int32, (rank, LANES), 1)
    ).astype(jnp.float32)

    def step(_, c):
        block = jnp.dot(bt_ref[...], gram[...], precision=HIGHEST, preferred_element_type=jnp.float32)
        wide[LANES - rank:, :] = block
        small = lax.dot_general(
            block, wide[...], (((1,), (1,)), ((), ())), precision=HIGHEST, preferred_element_type=jnp.float32
        )
        lower_inv = inverse_lower(small + eye, rank)
        bt_ref[...] = jnp.dot(lower_inv, block, precision=HIGHEST, preferred_element_type=jnp.float32)
        return c

    lax.fori_loop(0, ITERS, step, 0)
    basis = bt_ref[...].T
    height, cells = basis.shape[0] // parts, f_ref.shape[0] // parts
    for p in range(parts):
        f_ref[p * cells:(p + 1) * cells, :] = basis[p * height:p * height + cells, :]


def iterate(packed, start_basis, m, parts):
    cells, rank = start_basis.shape
    size = m * LANES
    start = start_basis.T.reshape(rank, parts, cells // parts)
    start = jnp.pad(start, ((0, 0), (0, 0), (0, (size - cells) // parts))).reshape(rank, size)
    vmem = pl.BlockSpec(memory_space=pltpu.VMEM)
    return pl.pallas_call(
        functools.partial(iterate_kernel, m, rank, parts),
        out_shape=(
            jax.ShapeDtypeStruct((rank, size), jnp.float32),
            jax.ShapeDtypeStruct((cells, rank), jnp.float32),
        ),
        in_specs=[vmem, vmem],
        out_specs=(vmem, vmem),
        scratch_shapes=[
            pltpu.VMEM((size, size), jnp.float32),
            pltpu.VMEM((LANES, size), jnp.float32),
        ],
    )(packed, start)


def core_kernel(axes, nv, bt_ref, x_ref, out_ref, xbuf, share, recv, local_sem, send_sem, recv_sem):
    units, size = xbuf.shape[0], xbuf.shape[1]
    na, steps, ranks = share.shape[0], recv_sem.shape[0], share.shape[2]
    width = units // steps
    nj2 = units // nv
    a = lax.axis_index(axes[0])
    rest = tuple(lax.axis_index(name) for name in axes[1:])

    def peer(k):
        return lax.rem(a + k, na)

    def dev(k):
        return (peer(k),) + rest

    def load(c):
        at = pl.ds(c * width, width)
        return pltpu.make_async_copy(x_ref.at[at], xbuf.at[at], local_sem.at[c])

    def go(c, k, came):
        at = pl.ds(c * width, width)
        sems = (send_sem.at[c, k], recv_sem.at[c, k])
        return send(share.at[peer(k), at], recv.at[came, at], sems, dev(k))

    def start(c, x):
        load(c).start()
        return x

    lax.fori_loop(0, steps, start, 0)
    greet([(na, dev)])
    bt = bt_ref[...]
    bt_hi = bt.astype(jnp.bfloat16)
    bt_lo = (bt - bt_hi.astype(jnp.float32)).astype(jnp.bfloat16)
    both = jnp.concatenate([bt_hi, bt_lo], axis=0)
    rank = bt.shape[0]

    def mul(c, x):
        load(c).wait()
        x = jnp.concatenate([xbuf[c * width + u] for u in range(width)], axis=1)
        hi = x.astype(jnp.bfloat16)
        lo = (x - hi.astype(jnp.float32)).astype(jnp.bfloat16)
        y = jnp.dot(both, hi, preferred_element_type=jnp.float32)
        y = y[:rank] + y[rank:] + jnp.dot(bt_hi, lo, preferred_element_type=jnp.float32)
        for p in range(na):
            for u in range(width):
                share[p, c * width + u] = y[p * ranks:(p + 1) * ranks, u * LANES:(u + 1) * LANES]

        @pl.when(c > 0)
        def _():
            for k in range(1, na):
                go(c - 1, k, a).start()

        return 0

    lax.fori_loop(0, steps, mul, 0)
    for k in range(1, na):
        go(steps - 1, k, a).start()
    stride = nv * na * nj2

    def place(c, x):
        for k in range(na):
            came = lax.rem(a + na - k, na)
            if k:
                go(c, k, came).wait_recv()
            for u in range(width):
                unit = c * width + u
                row = lax.div(unit, nj2) * (na * nj2) + came * nj2 + lax.rem(unit, nj2)
                value = recv[came, unit] if k else share[a, unit]
                out_ref[pl.ds(row, ranks, stride=stride), :] = value
        return x

    lax.fori_loop(0, steps, place, 0)

    def finish(c, x):
        for k in range(1, na):
            go(c, k, a).wait_send()
        return x

    lax.fori_loop(0, steps, finish, 0)


def core_of(basis_t, swapped, nv, axes, sizes):
    na = sizes[0]
    units, size, _ = swapped.shape
    ranks = basis_t.shape[0] // na
    width = 2 if units % 2 == 0 else 1
    steps = units // width
    vmem = pl.BlockSpec(memory_space=pltpu.VMEM)
    dma = pltpu.SemaphoreType.DMA
    return pl.pallas_call(
        functools.partial(core_kernel, axes, nv),
        out_shape=jax.ShapeDtypeStruct((ranks * units * na, LANES), jnp.float32),
        in_specs=[vmem, pl.BlockSpec(memory_space=pl.ANY)],
        out_specs=vmem,
        scratch_shapes=[
            pltpu.VMEM((units, size, LANES), jnp.float32),
            pltpu.VMEM((na, units, ranks, LANES), jnp.float32),
            pltpu.VMEM((na, units, ranks, LANES), jnp.float32),
            dma((steps,)),
            dma((steps, na)),
            dma((steps, na)),
        ],
        compiler_params=pltpu.CompilerParams(collective_id=2, has_side_effects=True),
    )(basis_t, swapped)


def solution(mesh):
    axes = tuple(mesh.axis_names)
    sizes = tuple(mesh.shape[a] for a in axes)

    def per_device(fields, var_scale, start_basis):
        na = sizes[0]
        nv, cells, nj, nk = fields.shape
        height = -(-cells // LANES) * LANES
        swapped, packed = swap_and_gram(fields, var_scale, height, axes, sizes)
        packed = all_reduce_rows(packed, axes, sizes)
        basis_t, factor = iterate(packed, start_basis, na * height // LANES, na)
        core = core_of(basis_t, swapped.reshape(-1, na * height, nk), nv, axes, sizes)
        core = core.reshape(-1, nv, nj, nk)
        return factor, core

    in_specs = (P(None, "gx", "gy", "gz"), P(), P())
    out_specs = (P(), P("gx", None, "gy", "gz"))
    return jax.shard_map(
        per_device, mesh=mesh, in_specs=in_specs, out_specs=out_specs, check_vma=False
    )
```

```python
import functools

import jax
import jax.numpy as jnp
from jax import lax
from jax.experimental import pallas as pl
from jax.experimental.pallas import tpu as pltpu
from jax.sharding import PartitionSpec as P

ITERS = 3
LANES = 128
SUB = 8
PANEL = 8
HIGHEST = lax.Precision.HIGHEST
MESH = pl.DeviceIdType.MESH


def flat_index(axes, sizes):
    flat = 0
    for name, size in zip(axes, sizes):
        flat = flat * size + lax.axis_index(name)
    return flat


def coords(flat, sizes):
    out = []
    for size in reversed(sizes):
        out.append(lax.rem(flat, size))
        flat = lax.div(flat, size)
    return tuple(reversed(out))


def greet(peers):
    barrier = pltpu.get_barrier_semaphore()
    for count, place in peers:
        for k in range(1, count):
            pl.semaphore_signal(barrier, inc=1, device_id=place(k), device_id_type=MESH)
    pl.semaphore_wait(barrier, sum(count - 1 for count, _ in peers))


def send(src, dst, sems, device):
    return pltpu.make_async_remote_copy(
        src_ref=src,
        dst_ref=dst,
        send_sem=sems[0],
        recv_sem=sems[1],
        device_id=device,
        device_id_type=MESH,
    )


def reduce_kernel(axes, sizes, g_ref, out_ref, recv_a, mine, recv_b, own, *sems):
    na, nb = g_ref.shape[0], g_ref.shape[1]
    rest = sizes[1:]
    a = lax.axis_index(axes[0])
    b = flat_index(axes[1:], rest)
    b_at = tuple(lax.axis_index(name) for name in axes[1:])

    def peer_a(k):
        return lax.rem(a + k, na)

    def peer_b(k):
        return lax.rem(b + k, nb)

    def dev_a(k):
        return (peer_a(k),) + b_at

    def dev_b(k):
        return (a,) + coords(peer_b(k), rest)

    greet([(na, dev_a), (nb, dev_b)])
    (s1, r1), (s2, r2), (s3, r3), (s4, r4) = [(sems[2 * i], sems[2 * i + 1]) for i in range(4)]

    order = list(range(1, nb)) + [0]
    first = {
        (k, q): send(g_ref.at[peer_a(k), peer_b(q)], recv_a.at[k, q], (s1.at[k, q], r1.at[k, q]), dev_a(k))
        for q in order
        for k in range(1, na)
    }
    for copy in first.values():
        copy.start()
    second = {
        q: send(mine.at[q], recv_b.at[q], (s2.at[q], r2.at[q]), dev_b(q)) for q in range(1, nb)
    }
    for q in order:
        for k in range(1, na):
            first[k, q].wait_recv()
        total = g_ref[a, peer_b(q)]
        for k in range(1, na):
            total = total + recv_a[k, q]
        mine[q] = total
        if q:
            second[q].start()
    for q in range(1, nb):
        second[q].wait_recv()
        total = total + recv_b[q]
    own[...] = total
    out_ref[a, b] = total

    third = [send(own, out_ref.at[a, b], (s3.at[q], r3.at[q]), dev_b(q)) for q in range(1, nb)]
    for copy in third:
        copy.start()
    fourth = []
    for q in range(nb):
        came = lax.rem(b + nb - q, nb)
        if q:
            send(own, out_ref.at[a, came], (s3.at[q], r3.at[q]), dev_b(q)).wait_recv()
        for k in range(1, na):
            block = own if q == 0 else out_ref.at[a, came]
            fourth.append(send(block, out_ref.at[a, came], (s4.at[k, q], r4.at[k, q]), dev_a(k)))
            fourth[-1].start()
    for q in range(nb):
        came = lax.rem(b + nb - q, nb)
        for k in range(1, na):
            came_a = lax.rem(a + na - k, na)
            send(own, out_ref.at[came_a, came], (s4.at[k, q], r4.at[k, q]), dev_a(k)).wait_recv()
    for copy in list(first.values()) + list(second.values()) + third + fourth:
        copy.wait_send()


def all_reduce_rows(packed, axes, sizes):
    na = sizes[0]
    nb = 1
    for size in sizes[1:]:
        nb *= size
    rows = packed.shape[0] // (na * nb)
    block = (rows, LANES)
    dma = pltpu.SemaphoreType.DMA
    out = pl.pallas_call(
        functools.partial(reduce_kernel, axes, sizes),
        out_shape=jax.ShapeDtypeStruct((na, nb) + block, jnp.float32),
        in_specs=[pl.BlockSpec(memory_space=pltpu.VMEM)],
        out_specs=pl.BlockSpec(memory_space=pltpu.VMEM),
        scratch_shapes=[
            pltpu.VMEM((na, nb) + block, jnp.float32),
            pltpu.VMEM((nb,) + block, jnp.float32),
            pltpu.VMEM((nb,) + block, jnp.float32),
            pltpu.VMEM(block, jnp.float32),
            dma((na, nb)), dma((na, nb)), dma((nb,)), dma((nb,)),
            dma((nb,)), dma((nb,)), dma((na, nb)), dma((na, nb)),
        ],
        compiler_params=pltpu.CompilerParams(collective_id=0, has_side_effects=True),
    )(packed.reshape((na, nb) + block))
    return out.reshape(na * nb * rows, LANES)


def swap_kernel(axes, chunk, cells, f_ref, scale_ref, buf, g_ref, acc, fbuf, t_ref, load_sem, local_sem, send_sem, recv_sem):
    units, na, height = buf.shape[0], buf.shape[1], buf.shape[2]
    size = na * height
    m = size // LANES
    chunks = units // chunk
    a = lax.axis_index(axes[0])
    rest = tuple(lax.axis_index(name) for name in axes[1:])

    def peer(k):
        return lax.rem(a + k, na)

    def dev(k):
        return (peer(k),) + rest

    def go(c, k):
        return send(
            t_ref.at[c, pl.ds(peer(k) * chunk, chunk)],
            buf.at[pl.ds(c * chunk, chunk), a],
            (send_sem.at[c, k], recv_sem.at[c, k]),
            dev(k),
        )

    def come(c, k):
        return send(
            t_ref.at[c, pl.ds(a * chunk, chunk)],
            buf.at[pl.ds(c * chunk, chunk), lax.rem(a + na - k, na)],
            (send_sem.at[c, k], recv_sem.at[c, k]),
            dev(k),
        )

    def stay(c):
        return pltpu.make_async_copy(
            t_ref.at[c, pl.ds(a * chunk, chunk)],
            buf.at[pl.ds(c * chunk, chunk), a],
            local_sem.at[c],
        )

    nj = na * chunk

    def load(c):
        return pltpu.make_async_copy(f_ref.at[c], fbuf.at[c], load_sem.at[c])

    def fetch(c, x):
        load(c).start()
        return x

    lax.fori_loop(0, chunks, fetch, 0)
    greet([(na, dev)])

    def start(c):
        for k in range(1, na):
            go(c, k).start()
        stay(c).start()

    def turn(c, x):
        load(c).wait()
        scale = scale_ref[c]
        for j in range(nj):
            t_ref[c, j, :cells, :] = fbuf[c, pl.ds(j, cells, stride=nj), :] * scale
            if cells < height:
                t_ref[c, j, cells:, :] = jnp.zeros((height - cells, LANES), jnp.float32)
        pl.when(c > 0)(lambda: start(c - 1))
        return x

    lax.fori_loop(0, chunks, turn, 0)
    start(chunks - 1)
    acc[...] = jnp.zeros_like(acc)

    def use(c, x):
        for k in range(1, na):
            come(c, k).wait_recv()
        stay(c).wait()
        x = jnp.concatenate(
            [buf[c * chunk + u].reshape(size, LANES) for u in range(chunk)], axis=1
        )
        for i in range(0, m, 2):
            top, low = i * LANES, min(i + 2, m) * LANES
            acc[top:low, top:] += lax.dot_general(
                x[top:low], x[top:], (((1,), (1,)), ((), ())),
                precision=HIGHEST, preferred_element_type=jnp.float32,
            )
        return 0

    lax.fori_loop(0, chunks, use, 0)
    t = 0
    for i in range(m):
        for j in range(i, m):
            g_ref[t * LANES:(t + 1) * LANES, :] = acc[
                i * LANES:(i + 1) * LANES, j * LANES:(j + 1) * LANES
            ]
            t += 1
    if t * LANES < g_ref.shape[0]:
        g_ref[t * LANES:, :] = jnp.zeros((g_ref.shape[0] - t * LANES, LANES), jnp.float32)

    def finish(c, x):
        for k in range(1, na):
            go(c, k).wait_send()
        return x

    lax.fori_loop(0, chunks, finish, 0)


def swap_and_gram(fields, var_scale, height, axes, sizes):
    na = sizes[0]
    n = 1
    for size in sizes:
        n *= size
    nv, cells, nj, nk = fields.shape
    chunk = nj // na
    units = nv * chunk
    m = na * height // LANES
    rows = -(-(m * (m + 1) // 2 * LANES) // (n * SUB)) * SUB
    vmem = pl.BlockSpec(memory_space=pltpu.VMEM)
    dma = pltpu.SemaphoreType.DMA
    return pl.pallas_call(
        functools.partial(swap_kernel, axes, chunk, cells),
        out_shape=(
            jax.ShapeDtypeStruct((units, na, height, LANES), jnp.float32),
            jax.ShapeDtypeStruct((n * rows, LANES), jnp.float32),
        ),
        in_specs=[pl.BlockSpec(memory_space=pl.ANY), pl.BlockSpec(memory_space=pltpu.SMEM)],
        out_specs=(vmem, vmem),
        scratch_shapes=[
            pltpu.VMEM((na * height, na * height), jnp.float32),
            pltpu.VMEM((nv, cells * nj, LANES), jnp.float32),
            pltpu.VMEM((nv, nj, height, LANES), jnp.float32),
            dma((nv,)),
            dma((nv,)),
            dma((nv, na)),
            dma((nv, na)),
        ],
        compiler_params=pltpu.CompilerParams(collective_id=1, has_side_effects=True),
    )(fields.reshape(nv, cells * nj, nk), var_scale)


def full(x):
    return jnp.broadcast_to(x, (SUB, LANES))


def inverse_lower(m, rank):
    groups = rank // SUB
    left = LANES - rank
    tiles = [m[g * SUB:(g + 1) * SUB, :] for g in range(groups)]
    sub = lax.broadcasted_iota(jnp.int32, (SUB, LANES), 0)
    done = []
    for g0 in range(groups):
        base = g0 * SUB
        cols = [
            [full(tiles[g][:, left + base + k:left + base + k + 1]) for g in range(g0, groups)]
            for k in range(SUB)
        ]
        rows = [full(tiles[g0][k:k + 1, :]) for k in range(SUB)]
        out = jnp.zeros((SUB, LANES), jnp.float32)
        for a in range(SUB):
            pivot = full(cols[a][0][a:a + 1, :])
            inv = 1.0 / pivot
            row = rows[a] * inv
            out = jnp.where(sub == a, rows[a] * lax.rsqrt(pivot), out)
            for b in range(a + 1, SUB):
                f = full(cols[a][0][b:b + 1, :])
                rows[b] = rows[b] - f * row
                fi = f * inv
                cols[b] = [cb - ca * fi for cb, ca in zip(cols[b], cols[a])]
            for i, g in enumerate(range(g0 + 1, groups)):
                tiles[g] = tiles[g] - cols[a][i + 1] * row
        done.append(out)
    return jnp.concatenate(done, axis=0)[:, :rank]


def iterate_kernel(m, rank, parts, p_ref, start_ref, bt_ref, f_ref, gram, wide):
    t = 0
    for i in range(m):
        for j in range(i, m):
            block = p_ref[t * LANES:(t + 1) * LANES, :]
            gram[i * LANES:(i + 1) * LANES, j * LANES:(j + 1) * LANES] = block
            if i != j:
                gram[j * LANES:(j + 1) * LANES, i * LANES:(i + 1) * LANES] = block.T
            t += 1
    wide[...] = jnp.zeros_like(wide)
    bt_ref[...] = start_ref[...]
    eye = (
        lax.broadcasted_iota(jnp.int32, (rank, LANES), 0)
        == lax.broadcasted_iota(jnp.int32, (rank, LANES), 1)
    ).astype(jnp.float32)

    def step(_, c):
        block = jnp.dot(bt_ref[...], gram[...], precision=HIGHEST, preferred_element_type=jnp.float32)
        wide[LANES - rank:, :] = block
        small = lax.dot_general(
            block, wide[...], (((1,), (1,)), ((), ())), precision=HIGHEST, preferred_element_type=jnp.float32
        )
        lower_inv = inverse_lower(small + eye, rank)
        bt_ref[...] = jnp.dot(lower_inv, block, precision=HIGHEST, preferred_element_type=jnp.float32)
        return c

    lax.fori_loop(0, ITERS, step, 0)
    height, cells = bt_ref.shape[1] // parts, f_ref.shape[1] // parts
    f_ref[...] = jnp.concatenate(
        [bt_ref[:, p * height:p * height + cells] for p in range(parts)], axis=1
    )


def iterate(packed, start_basis, m, parts):
    cells, rank = start_basis.shape
    size = m * LANES
    start = start_basis.T.reshape(rank, parts, cells // parts)
    start = jnp.pad(start, ((0, 0), (0, 0), (0, (size - cells) // parts))).reshape(rank, size)
    vmem = pl.BlockSpec(memory_space=pltpu.VMEM)
    return pl.pallas_call(
        functools.partial(iterate_kernel, m, rank, parts),
        out_shape=(
            jax.ShapeDtypeStruct((rank, size), jnp.float32),
            jax.ShapeDtypeStruct((rank, cells), jnp.float32),
        ),
        in_specs=[vmem, vmem],
        out_specs=(vmem, vmem),
        scratch_shapes=[
            pltpu.VMEM((size, size), jnp.float32),
            pltpu.VMEM((LANES, size), jnp.float32),
        ],
    )(packed, start)


def core_kernel(axes, nv, bt_ref, x_ref, out_ref, xbuf, share, recv, local_sem, send_sem, recv_sem):
    units, size = xbuf.shape[0], xbuf.shape[1]
    na, steps, ranks = share.shape[0], recv_sem.shape[0], share.shape[2]
    width = units // steps
    nj2 = units // nv
    a = lax.axis_index(axes[0])
    rest = tuple(lax.axis_index(name) for name in axes[1:])

    def peer(k):
        return lax.rem(a + k, na)

    def dev(k):
        return (peer(k),) + rest

    def load(c):
        at = pl.ds(c * width, width)
        return pltpu.make_async_copy(x_ref.at[at], xbuf.at[at], local_sem.at[c])

    def go(c, k, came):
        at = pl.ds(c * width, width)
        sems = (send_sem.at[c, k], recv_sem.at[c, k])
        return send(share.at[peer(k), at], recv.at[came, at], sems, dev(k))

    def start(c, x):
        load(c).start()
        return x

    lax.fori_loop(0, steps, start, 0)
    greet([(na, dev)])
    bt = bt_ref[...]
    bt_hi = bt.astype(jnp.bfloat16)
    bt_lo = (bt - bt_hi.astype(jnp.float32)).astype(jnp.bfloat16)
    both = jnp.concatenate([bt_hi, bt_lo], axis=0)
    rank = bt.shape[0]

    def mul(c, x):
        load(c).wait()
        x = jnp.concatenate([xbuf[c * width + u] for u in range(width)], axis=1)
        hi = x.astype(jnp.bfloat16)
        lo = (x - hi.astype(jnp.float32)).astype(jnp.bfloat16)
        y = jnp.dot(both, hi, preferred_element_type=jnp.float32)
        y = y[:rank] + y[rank:] + jnp.dot(bt_hi, lo, preferred_element_type=jnp.float32)
        for p in range(na):
            for u in range(width):
                share[p, c * width + u] = y[p * ranks:(p + 1) * ranks, u * LANES:(u + 1) * LANES]

        @pl.when(c > 0)
        def _():
            for k in range(1, na):
                go(c - 1, k, a).start()

        return 0

    lax.fori_loop(0, steps, mul, 0)
    for k in range(1, na):
        go(steps - 1, k, a).start()
    stride = nv * na * nj2

    def place(c, x):
        for k in range(na):
            came = lax.rem(a + na - k, na)
            if k:
                go(c, k, came).wait_recv()
            for u in range(width):
                unit = c * width + u
                row = lax.div(unit, nj2) * (na * nj2) + came * nj2 + lax.rem(unit, nj2)
                value = recv[came, unit] if k else share[a, unit]
                out_ref[pl.ds(row, ranks, stride=stride), :] = value
        return x

    lax.fori_loop(0, steps, place, 0)

    def finish(c, x):
        for k in range(1, na):
            go(c, k, a).wait_send()
        return x

    lax.fori_loop(0, steps, finish, 0)


def core_of(basis_t, swapped, nv, axes, sizes):
    na = sizes[0]
    units, size, _ = swapped.shape
    ranks = basis_t.shape[0] // na
    width = 2 if units % 2 == 0 else 1
    steps = units // width
    vmem = pl.BlockSpec(memory_space=pltpu.VMEM)
    dma = pltpu.SemaphoreType.DMA
    return pl.pallas_call(
        functools.partial(core_kernel, axes, nv),
        out_shape=jax.ShapeDtypeStruct((ranks * units * na, LANES), jnp.float32),
        in_specs=[vmem, pl.BlockSpec(memory_space=pl.ANY)],
        out_specs=vmem,
        scratch_shapes=[
            pltpu.VMEM((units, size, LANES), jnp.float32),
            pltpu.VMEM((na, units, ranks, LANES), jnp.float32),
            pltpu.VMEM((na, units, ranks, LANES), jnp.float32),
            dma((steps,)),
            dma((steps, na)),
            dma((steps, na)),
        ],
        compiler_params=pltpu.CompilerParams(collective_id=2, has_side_effects=True),
    )(basis_t, swapped)


def solution(mesh):
    axes = tuple(mesh.axis_names)
    sizes = tuple(mesh.shape[a] for a in axes)

    def per_device(fields, var_scale, start_basis):
        na = sizes[0]
        nv, cells, nj, nk = fields.shape
        height = -(-cells // LANES) * LANES
        swapped, packed = swap_and_gram(fields, var_scale, height, axes, sizes)
        packed = all_reduce_rows(packed, axes, sizes)
        basis_t, factor = iterate(packed, start_basis, na * height // LANES, na)
        core = core_of(basis_t, swapped.reshape(-1, na * height, nk), nv, axes, sizes)
        core = core.reshape(-1, nv, nj, nk)
        return factor.T, core

    in_specs = (P(None, "gx", "gy", "gz"), P(), P())
    out_specs = (P(), P("gx", None, "gy", "gz"))
    return jax.shard_map(
        per_device, mesh=mesh, in_specs=in_specs, out_specs=out_specs, check_vma=False
    )
```
